32 devices in a mesh: comp: 2 (over x), tile: 16 (over z, y, core).
Axes of the slice: x: 2, y: 2, z: 4, core: 2. Of those that a mesh axis runs over, the one named last changes fastest.
Arguments:
- starting_perturbation: float32 [2, 128, 128, 512], P('comp', None, 'tile'), may hold values from -6 to 6
- measured_discrepancy: float32 [2, 128, 128, 512], P('comp', None, 'tile'), may hold values from -6 to 6
- diffusion: float32 [2, 128, 128, 512], P('comp', None, 'tile'), may hold values from 0.02 to 0.24
- vert_mix: float32 [2, 128, 128], P('comp'), may hold values from -0.03125 to 0.03125
- ocean_mask: int32 [128, 512], P('tile'), may hold values 0 or 1
- pair_tile: int32 [2, 16, 8], replicated, may hold values from 0 to 15, as said below
- pair_patch: int32 [2, 16, 64], replicated, may hold values from 0 to 31
- dest_patch: int32 [2, 16, 64], P('comp', 'tile'), may hold values from 0 to 31
- pair_blocks: int32 [2, 16, 8], P('comp', 'tile'), may hold values from 1 to 8, 48 in all within a row
- remap_weight: float32 [2, 1024, 128, 128], P('comp', 'tile'), may hold values from -0.5 to 0.5
Outputs:
- final_perturbation: float32 [2, 128, 128, 512], P('comp', None, 'tile')
- gradient: float32 [2, 128, 128, 512], P('comp', None, 'tile')
The draws below stay inside these ranges and needn't reach their ends.
Inputs may be any that keep to these rules, and one draw needn't show every extreme that they name: `pair_tile`: the 8 source tiles listed for destination tile t are distinct; exactly one of them is (t + 8) mod 16, and each other is (t + o) mod 16 for some o from 1 - 8 to 7. A pair's live blocks are its first pair_blocks ones.
All inputs are finite; a program needn't handle non-finite values. No bound on the sum of `ocean_mask` on one device may be relied on, other than what follows from the above.
Results may differ from the reference program's by a relative error of at most 0.0001.
Values sent between devices are 32-bit elements; how exact they have to be, the bound alone decides.
A program may use at most 128 MiB of HBM per device.

```python
import math
import jax
import jax.numpy as jnp
import numpy as np
from jax import lax

LEV = 128
LON = 512
STEPS = 4
NPAIR = 8
PB = 8
PATCH = 128
TILES = 16
NROWS = 128
NBLK = 64
NPATCH = 32


def draw_pair_tile(key, part):
    key_list = jax.random.split(jax.random.fold_in(key, 17), 2 * TILES)
    tile_ids = jnp.tile(jnp.arange(TILES, dtype=jnp.int32), 2)

    def draw_row(subkey, tile_now):
        first_key, second_key = jax.random.split(subkey)
        near_offsets = jax.random.permutation(first_key, 2 * NPAIR - 1)[:NPAIR - 1].astype(jnp.int32) - (NPAIR - 1)
        all_offsets = jnp.concatenate([near_offsets, jnp.full((1,), TILES // 2, jnp.int32)])
        ordered = jax.random.permutation(second_key, all_offsets)
        return (tile_now + ordered) % TILES
    return jax.vmap(draw_row)(key_list, tile_ids).reshape(2, TILES, NPAIR).astype(jnp.int32)


def set_ends(values, own_key, smallest, high):
    longest = values.shape.index(max(values.shape))
    spots = []
    for shift in (0, 1):
        where = [jax.random.randint(jax.random.fold_in(own_key, axis), (), 0, length) for axis, length in enumerate(values.shape)]
        where[longest] = (where[longest] + shift) % values.shape[longest]
        spots.append(tuple(where))
    return values.at[spots[0]].set(smallest).at[spots[1]].set(high)


def levels(stream_key, dims, cuts, smallest, top_value):
    level = 1.0
    for axis_at, shards_of in cuts:
        draws = jax.random.uniform(jax.random.fold_in(jax.random.fold_in(stream_key, 6), axis_at), (shards_of,), jnp.float32, smallest / len(cuts), top_value / len(cuts))
        level = level * jnp.repeat(jnp.exp(draws), dims[axis_at] // shards_of).reshape((-1,) + (1,) * (len(dims) - 1 - axis_at))
    return level


def profile(count, total, most, skew):
    weights = [(1 << 20) // math.isqrt(grade ** skew) + 1 for grade in range(2, count + 1)]
    surplus, holding = total - most - (count - 1), [1] * (count - 1)
    while surplus > 0:
        free = [i for i in range(count - 1) if holding[i] < most]
        whole, remaining = sum([weights[i] for i in free]), surplus
        for i in free:
            extra = min(most - holding[i], max(1, remaining * weights[i] // whole), surplus)
            holding[i] = holding[i] + extra
            surplus = surplus - extra
    return np.array([most] + holding)


def ragged(key, count, total, limit, lean):
    if count == 2:
        one = jax.random.randint(key, (), max(1, total - limit), min(limit, total - 1) + 1)
        return jnp.stack([one, total - one])
    lengths = jnp.asarray(profile(count, total, limit, lean), jnp.int32)
    couples = (count - 1) // 2
    giver, sink = lengths[1:1 + 2 * couples:2], lengths[2:2 + 2 * couples:2]
    room = jnp.minimum(giver - 1, limit - sink)
    moved = jax.random.randint(jax.random.fold_in(key, 1), (couples,), 0, 1 << 20) % (room + 1)
    lengths = lengths.at[1:1 + 2 * couples:2].set(giver - moved).at[2:2 + 2 * couples:2].set(sink + moved)
    return lengths[jax.random.permutation(jax.random.fold_in(key, 2), count)]


def gaussian(rng, dims, deviation, limit, cuts=(), kind=jnp.bfloat16):
    level = levels(rng, dims, cuts, -0.22, 0.18) if cuts else 1.0
    drawn = jax.random.normal(rng, dims, jnp.float32) * deviation * level
    return jnp.minimum(jnp.maximum(drawn, -limit), limit).astype(kind)


def setup_inputs(seed: int = 0) -> dict:
    splits = jax.random.split(jax.random.key(seed), 11)
    starting_perturbation = gaussian(splits[0], (2, LEV, NROWS, LON), 1.0, 6.0, ((0, 2), (2, 16)), jnp.float32)
    measured_discrepancy = gaussian(splits[1], (2, LEV, NROWS, LON), 1.0, 6.0, ((0, 2), (2, 16)), jnp.float32)
    diffusion = jnp.clip(jnp.exp(math.log(0.24) - 2.4849066 * jax.random.uniform(splits[2], (2, LEV, NROWS, LON), jnp.float32) ** levels(splits[2], (2, LEV, NROWS, LON), ((0, 2), (2, 16)), -0.2, 0.2)), 0.02, 0.24)
    vert_mix = gaussian(splits[3], (2, LEV, LEV), (256 * LEV) ** -0.5, 0.03125, ((0, 2),), jnp.float32)
    ocean_mask = set_ends((jax.random.randint(splits[4], (NROWS, LON), 0, 10) < 7).astype(jnp.int32), jax.random.fold_in(splits[4], 1), 0, 1)
    pair_tile = draw_pair_tile(jax.random.fold_in(splits[10], 71), 0)
    pair_patch = set_ends(jax.random.randint(splits[6], (2, TILES, NBLK), 0, NPATCH), jax.random.fold_in(splits[6], 1), 0, NPATCH - 1).astype(jnp.int32)
    dest_patch = set_ends(jax.random.randint(splits[7], (2, TILES, NBLK), 0, NPATCH), jax.random.fold_in(splits[7], 1), 0, NPATCH - 1).astype(jnp.int32)
    pair_blocks = jax.vmap(lambda own: ragged(own, NPAIR, NPAIR * PB * 3 // 4, PB, 2))(jax.random.split(splits[8], 2 * TILES)).reshape((2, TILES, NPAIR)).astype(jnp.int32)
    remap_weight = gaussian(splits[9], (2, TILES * NBLK, PATCH, PATCH), PATCH ** -0.5, 0.5, ((0, 2), (1, 16)), jnp.float32)
    return dict(starting_perturbation=starting_perturbation, measured_discrepancy=measured_discrepancy, diffusion=diffusion, vert_mix=vert_mix, ocean_mask=ocean_mask, pair_tile=pair_tile, pair_patch=pair_patch, dest_patch=dest_patch, pair_blocks=pair_blocks, remap_weight=remap_weight)


precise = lax.Precision.HIGHEST

def laplace(system_variables):
    padded = jnp.pad(system_variables, ((0, 0), (0, 0), (1, 1), (0, 0)))
    return padded[:, :, 2:] + padded[:, :, :-2] + jnp.roll(system_variables, -1, axis=3) + jnp.roll(system_variables, 1, axis=3) - 4.0 * system_variables

def column_mix(matrix, system_variables):
    return jnp.einsum('clm,cmrx->clrx', matrix, system_variables, precision=precise)

def reference(starting_perturbation, measured_discrepancy, diffusion, vert_mix, ocean_mask, pair_tile, pair_patch, dest_patch, pair_blocks, remap_weight):
    seawater_indicator = jnp.stack([jnp.ones((NROWS, LON), jnp.float32), ocean_mask.astype(jnp.float32)])[:, None]
    block_ids = jnp.arange(NBLK, dtype=jnp.int32)
    owner_pair = block_ids // PB
    slot_ids = block_ids % PB

    def remap(surface, destination):
        source = surface[1 - destination].reshape(TILES * NPATCH, PATCH)
        source_rows = (pair_tile[destination][:, owner_pair] * NPATCH + pair_patch[destination]).reshape(-1)
        live_mask = (slot_ids[None, :] < pair_blocks[destination][:, owner_pair]).astype(jnp.float32).reshape(-1, 1)
        block_terms = jnp.einsum('bij,bj->bi', remap_weight[destination], source[source_rows], precision=precise) * live_mask
        target = (jnp.arange(TILES, dtype=jnp.int32)[:, None] * NPATCH + dest_patch[destination]).reshape(-1)
        summed_sensitivity = jnp.zeros((TILES * NPATCH, PATCH), jnp.float32).at[target].add(block_terms)
        return summed_sensitivity.reshape(NROWS, LON)

    def couple(system_variables):
        surface = system_variables[:, 0]
        summed_sensitivity = jnp.stack([remap(surface, 0), remap(surface, 1)])
        return system_variables.at[:, 0].add(seawater_indicator[:, 0] * summed_sensitivity)

    def forward_step(system_variables):
        return seawater_indicator * (system_variables + diffusion * laplace(system_variables) + column_mix(vert_mix, system_variables))

    def joint_earth_system(system_variables):
        for step_index in range(STEPS):
            system_variables = forward_step(system_variables)
        system_variables = couple(system_variables)
        for step_index in range(STEPS):
            system_variables = forward_step(system_variables)
        return system_variables
    final_perturbation, reverse_derivative_operator = jax.vjp(joint_earth_system, starting_perturbation)
    measurement_mismatch = final_perturbation - measured_discrepancy
    backpropagated_sensitivity = reverse_derivative_operator(measurement_mismatch)[0]
    return (final_perturbation, starting_perturbation + backpropagated_sensitivity)
```

```python
import functools

import jax
import jax.numpy as jnp
from jax import lax
from jax.experimental import pallas as pl
from jax.experimental.pallas import tpu as pltpu
from jax.sharding import PartitionSpec as P

STEPS = 4
CHUNKS = 2
SUB = 32
MESH = pl.DeviceIdType.MESH
precise = lax.Precision.HIGHEST
f32, bf16 = jnp.float32, jnp.bfloat16


def split(x):
    high = x.astype(bf16)
    return high, (x - high.astype(f32)).astype(bf16)


def mix(a_wide, a_low, x):
    high, low = split(x)
    both = jnp.concatenate([high, low], axis=0)
    return jnp.dot(a_wide, both, preferred_element_type=f32) + jnp.dot(
        a_low, high, preferred_element_type=f32
    )


def block(tiles, forward, backward, *refs):
    refs = list(refs)
    x_hbm, d_ref, a_ref, sea_ref = refs[:4]
    del refs[:4]
    add_ref = refs.pop(0)
    measured = refs.pop(0) if forward and backward else None
    outs = [refs.pop(0) for _ in range(bool(forward) + bool(backward))]
    state, halo, send_sem, recv_sem, io_sem, wide, low = refs[:7]
    del refs[:7]
    masked, wide_t, low_t = refs if backward else (None,) * 3
    comp, me = lax.axis_index("comp"), lax.axis_index("tile")
    rows, levels, lon = d_ref.shape
    width = lon // CHUNKS
    up, down = lax.rem(me + tiles - 1, tiles), lax.rem(me + 1, tiles)
    has_up, has_down = me > 0, me < tiles - 1
    has = (has_up, has_down)

    first = masked if not forward else state.at[0]
    load = pltpu.make_async_copy(x_hbm, first, io_sem.at[0])
    load.start()

    barrier = pltpu.get_barrier_semaphore()
    for there, other in ((has_up, up), (has_down, down)):

        @pl.when(there)
        def _():
            pl.semaphore_signal(barrier, inc=1, device_id=(comp, other), device_id_type=MESH)

    if forward:
        high, rest = split(a_ref[...])
        wide[...] = jnp.concatenate([high, high], axis=1)
        low[...] = rest
    if backward:
        high, rest = split(a_ref[...].T)
        wide_t[...] = jnp.concatenate([high, high], axis=1)
        low_t[...] = rest
    total = forward + backward
    for side in (0, 1):

        @pl.when(jnp.logical_not(has[side]))
        def _():
            def clear(i, _):
                halo[i, side] = jnp.zeros((levels, lon), f32)
                return _

            lax.fori_loop(0, total, clear, 0)

    pl.semaphore_wait(barrier, has_up.astype(jnp.int32) + has_down.astype(jnp.int32))
    load.wait()
    for r in range(rows):
        first[r, 0:1, :] = first[r, 0:1, :] + add_ref[r : r + 1, :]

    def copy(h, slot, side, c):
        columns = pl.ds(c * width, width)
        return pltpu.make_async_remote_copy(
            src_ref=state.at[slot, (rows - 1) * side, :, columns],
            dst_ref=halo.at[h, 1 - side, :, columns],
            send_sem=send_sem.at[h, side, c],
            recv_sem=recv_sem.at[h, 1 - side, c],
            device_id=(comp, (up, down)[side]),
            device_id_type=MESH,
        )

    def send(h, slot, side, c):
        @pl.when(has[side])
        def _():
            copy(h, slot, side, c).start()

    def receive(h, slot, side, c):
        @pl.when(has[side])
        def _():
            copy(h, slot, 1 - side, c).wait_recv()

    def pieces():
        return [slice(k, k + SUB) for k in range(0, levels, SUB)]

    def stencil(now, above, below, k, cols):
        x = now[k, :]
        left, right = pltpu.roll(x, 1, axis=1), pltpu.roll(x, lon - 1, axis=1)
        around = (left + right)[:, cols] + (above[k, cols] + below[k, cols])
        return x[:, cols], around - 4.0 * x[:, cols]

    def forward_row(slot, r, above, below, cols, target):
        now = state.at[slot, r]
        sea = sea_ref[pl.ds(r, 1), :][:, cols]
        y = mix(wide[...], low[...], now[:, cols])
        for k in pieces():
            x, lap = stencil(now, above, below, k, cols)
            target[r, k, cols] = sea * (x + d_ref[r, k, cols] * lap + y[k])

    def scaled_row(slot, r, cols, k, adjoint):
        u = sea_ref[pl.ds(r, 1), :][:, cols] * adjoint
        masked[r, k, cols] = u
        state[slot, r, k, cols] = d_ref[r, k, cols] * u

    def backward_row(slot, r, above, below, cols, last):
        now = state.at[slot, r]
        y = mix(wide_t[...], low_t[...], masked[r, :, cols])
        for k in pieces():
            _, lap = stencil(now, above, below, k, cols)
            adjoint = masked[r, k, cols] + lap + y[k]
            if last:
                masked[r, k, cols] = adjoint
            else:
                scaled_row(slot + 1, r, cols, k, adjoint)

    every = slice(0, lon)

    def step(h, slot, row, more):
        def inner(r, _):
            row(slot, r, state.at[slot, r - 1], state.at[slot, r + 1], every)
            return _

        lax.fori_loop(1, rows - 1, inner, 0)
        for c in range(CHUNKS):
            cols = slice(c * width, (c + 1) * width)
            for side in (0, 1):
                receive(h, slot, side, c)
                if side == 0:
                    row(slot, 0, halo.at[h, 0], state.at[slot, 1], cols)
                else:
                    row(slot, rows - 1, state.at[slot, rows - 2], halo.at[h, 1], cols)
                if more:
                    send(h + 1, slot + 1, side, c)

    def all_edges(h, slot):
        for c in range(CHUNKS):
            for side in (0, 1):
                send(h, slot, side, c)

    def run(base, slot0, count, make):
        def one(i, _):
            step(base + i, slot0 + i, make(False), True)
            return _

        lax.fori_loop(0, count - 1, one, 0)
        step(base + count - 1, slot0 + count - 1, make(True), False)

    base = 0
    slot0 = 0
    stores = []
    if forward:
        all_edges(0, 0)

        def make(last):
            return lambda slot, r, above, below, cols: forward_row(
                slot, r, above, below, cols, state.at[slot + 1]
            )

        run(0, 0, forward, make)
        base, slot0 = forward, forward + 1
        stores.append(pltpu.make_async_copy(state.at[forward], outs[0], io_sem.at[1]))
        stores[-1].start()
    if backward:

        def start_row(r, _):
            for k in pieces():
                if forward:
                    value = state[forward, r, k, :] - measured[r, k, :]
                else:
                    value = masked[r, k, :]
                scaled_row(slot0, r, every, k, value)
            return _

        start_row(0, 0)
        start_row(rows - 1, 0)
        all_edges(base, slot0)
        lax.fori_loop(1, rows - 1, start_row, 0)

        def make(last):
            return lambda slot, r, above, below, cols: backward_row(
                slot, r, above, below, cols, last
            )

        run(base, slot0, backward, make)
        stores.append(pltpu.make_async_copy(masked, outs[-1], io_sem.at[2]))
        stores[-1].start()
    for side in (0, 1):

        @pl.when(has[side])
        def _():
            for h in range(total):
                slot = h if h < forward else h + bool(forward)
                for c in range(CHUNKS):
                    copy(h, slot, side, c).wait_send()

    for store in stores:
        store.wait()


def run_block(tiles, ident, forward, backward, x, d, a, sea, add, measured=None):
    rows, levels, lon = x.shape
    total = forward + backward
    slots = (forward + 1 if forward else 0) + backward
    vmem = pl.BlockSpec(memory_space=pltpu.VMEM)
    hbm = pl.BlockSpec(memory_space=pl.ANY)
    operands = [x, d, a, sea, add] + ([measured] if measured is not None else [])
    outs = bool(forward) + bool(backward)
    scratch = [
        pltpu.VMEM((slots, rows, levels, lon), f32),
        pltpu.VMEM((total, 2, levels, lon), f32),
        pltpu.SemaphoreType.DMA((total, 2, CHUNKS)),
        pltpu.SemaphoreType.DMA((total, 2, CHUNKS)),
        pltpu.SemaphoreType.DMA((3,)),
        pltpu.VMEM((levels, 2 * levels), bf16),
        pltpu.VMEM((levels, levels), bf16),
    ]
    if backward:
        scratch += [
            pltpu.VMEM((rows, levels, lon), f32),
            pltpu.VMEM((levels, 2 * levels), bf16),
            pltpu.VMEM((levels, levels), bf16),
        ]
    return pl.pallas_call(
        functools.partial(block, tiles, forward, backward),
        out_shape=[jax.ShapeDtypeStruct(x.shape, f32)] * outs,
        in_specs=[hbm] + [vmem] * (len(operands) - 1),
        out_specs=[hbm] * outs,
        scratch_shapes=scratch,
        compiler_params=pltpu.CompilerParams(
            collective_id=ident, has_side_effects=True, vmem_limit_bytes=56 * 2**20
        ),
    )(*operands)


def swap_kernel(tiles, parcel, out, slots, send_sem, recv_sem):
    other, me = 1 - lax.axis_index("comp"), lax.axis_index("tile")
    barrier = pltpu.get_barrier_semaphore()
    for t in range(tiles):
        pl.semaphore_signal(barrier, inc=1, device_id=(other, t), device_id_type=MESH)
    pl.semaphore_wait(barrier, tiles)

    def copy(k, goes, lands):
        return pltpu.make_async_remote_copy(
            src_ref=parcel.at[goes],
            dst_ref=slots.at[lands],
            send_sem=send_sem.at[k],
            recv_sem=recv_sem.at[k],
            device_id=(other, goes),
            device_id_type=MESH,
        )

    for k in range(tiles):
        copy(k, lax.rem(me + k, tiles), me).start()
    for k in range(tiles):
        copy(k, lax.rem(me + k, tiles), lax.rem(me + tiles - k, tiles)).wait_recv()
    out[...] = slots[...]
    for k in range(tiles):
        copy(k, lax.rem(me + k, tiles), me).wait_send()


def swap(tiles, ident, parcel):
    vmem = pl.BlockSpec(memory_space=pltpu.VMEM)
    return pl.pallas_call(
        functools.partial(swap_kernel, tiles),
        out_shape=jax.ShapeDtypeStruct(parcel.shape, f32),
        in_specs=[vmem],
        out_specs=vmem,
        scratch_shapes=[
            pltpu.VMEM(parcel.shape, f32),
            pltpu.SemaphoreType.DMA((tiles,)),
            pltpu.SemaphoreType.DMA((tiles,)),
        ],
        compiler_params=pltpu.CompilerParams(collective_id=ident, has_side_effects=True),
    )(parcel)


def one_hot(index, count):
    return (index[:, None] == jnp.arange(count, dtype=jnp.int32)[None, :]).astype(f32)


def shards(
    starting_perturbation,
    measured_discrepancy,
    diffusion,
    vert_mix,
    ocean_mask,
    pair_tile,
    pair_patch,
    dest_patch,
    pair_blocks,
    remap_weight,
):
    component = lax.axis_index("comp")
    own_tile = lax.axis_index("tile")
    tiles = lax.axis_size("tile")
    row_count = starting_perturbation.shape[2]
    lon_count = starting_perturbation.shape[3]
    patch_len = remap_weight.shape[2]
    patch_count = row_count * lon_count // patch_len
    block_count = remap_weight.shape[1]
    pair_count = pair_tile.shape[2]
    per_pair = block_count // pair_count
    partner = 1 - component
    sea = jnp.where(component == 1, ocean_mask.astype(f32), 1.0)
    slot_ids = jnp.arange(block_count, dtype=jnp.int32) % per_pair
    own_tiles = jnp.repeat(pair_tile[component, own_tile], per_pair)
    live = (slot_ids < jnp.repeat(pair_blocks[0, 0], per_pair)).astype(f32)[:, None]
    landing = one_hot(dest_patch[0, 0], patch_count) * live
    weights = remap_weight[0]
    hits = (pair_tile[partner] == own_tile).astype(jnp.int32)
    feed = pair_patch[partner].reshape(tiles, pair_count, per_pair)
    send_rows = jnp.sum(hits[:, :, None] * feed, axis=1)
    sent = jnp.sum(hits, axis=1).astype(f32)
    sending = one_hot(send_rows.reshape(-1), patch_count) * jnp.repeat(sent, per_pair)[:, None]
    taking = one_hot(own_tiles * per_pair + slot_ids, tiles * per_pair)

    def to_rows(x):
        return jnp.swapaxes(x[0], 0, 1)

    start, measured, diff = map(
        to_rows, (starting_perturbation, measured_discrepancy, diffusion)
    )
    none = jnp.zeros((row_count, lon_count), f32)
    (middle,) = run_block(tiles, 0, STEPS, 0, start, diff, vert_mix[0], sea, none)

    surface = middle[:, 0].reshape(patch_count, patch_len)
    parcel = jnp.dot(sending, surface, precision=precise)
    arrived = swap(tiles, 1, parcel.reshape(tiles, per_pair, patch_len))
    picked = jnp.dot(taking, arrived.reshape(tiles * per_pair, patch_len), precision=precise)
    terms = jnp.sum(weights * picked[:, None, :], axis=2)
    summed = jnp.dot(landing.T, terms, precision=precise).reshape(row_count, lon_count)
    final, adjoint = run_block(
        tiles, 2, STEPS, STEPS, middle, diff, vert_mix[0], sea, sea * summed, measured
    )

    masked = sea.reshape(patch_count, patch_len) * adjoint[:, 0].reshape(patch_count, patch_len)
    spread = jnp.dot(landing, masked, precision=precise)
    terms = jnp.sum(weights * spread[:, :, None], axis=1)
    parcel = jnp.dot(taking.T, terms, precision=precise)
    back = swap(tiles, 3, parcel.reshape(tiles, per_pair, patch_len))
    returned = jnp.dot(sending.T, back.reshape(tiles * per_pair, patch_len), precision=precise)
    (last,) = run_block(
        tiles,
        4,
        0,
        STEPS,
        adjoint,
        diff,
        vert_mix[0],
        sea,
        returned.reshape(row_count, lon_count),
    )
    gradient = starting_perturbation + jnp.swapaxes(last, 0, 1)[None]
    return (jnp.swapaxes(final, 0, 1)[None], gradient)


def solution(mesh):
    placed = (
        P("comp", None, "tile", None),
        P("comp", None, "tile", None),
        P("comp", None, "tile", None),
        P("comp", None, None),
        P("tile", None),
        P(),
        P(),
        P("comp", "tile", None),
        P("comp", "tile", None),
        P("comp", "tile", None, None),
    )
    return jax.shard_map(
        shards,
        mesh=mesh,
        in_specs=placed,
        out_specs=(P("comp", None, "tile", None), P("comp", None, "tile", None)),
        check_vma=False,
    )
```

```python
import functools

import jax
import jax.numpy as jnp
from jax import lax
from jax.experimental import pallas as pl
from jax.experimental.pallas import tpu as pltpu
from jax.sharding import PartitionSpec as P

STEPS = 4
CHUNKS = 4
SUB = 32
MESH = pl.DeviceIdType.MESH
precise = lax.Precision.HIGHEST
f32, bf16 = jnp.float32, jnp.bfloat16


def split(x):
    high = x.astype(bf16)
    return high, (x - high.astype(f32)).astype(bf16)


def mix(a_wide, a_low, x):
    high, low = split(x)
    both = jnp.concatenate([high, low], axis=0)
    return jnp.dot(a_wide, both, preferred_element_type=f32) + jnp.dot(
        a_low, high, preferred_element_type=f32
    )


def block(tiles, forward, backward, *refs):
    refs = list(refs)
    x_hbm, d_ref, a_ref, sea_ref = refs[:4]
    del refs[:4]
    add_ref = refs.pop(0)
    extra = refs.pop(0) if backward else None
    outs = [refs.pop(0) for _ in range(bool(forward) + bool(backward))]
    state, halo, send_sem, recv_sem, io_sem, wide, low = refs[:7]
    del refs[:7]
    masked, wide_t, low_t = refs if backward else (None,) * 3
    comp, me = lax.axis_index("comp"), lax.axis_index("tile")
    rows, levels, lon = d_ref.shape
    width = lon // CHUNKS
    up, down = lax.rem(me + tiles - 1, tiles), lax.rem(me + 1, tiles)
    has_up, has_down = me > 0, me < tiles - 1
    has = (has_up, has_down)

    first = masked if not forward else state.at[0]
    load = pltpu.make_async_copy(x_hbm, first, io_sem.at[0])
    load.start()

    barrier = pltpu.get_barrier_semaphore()
    for there, other in ((has_up, up), (has_down, down)):

        @pl.when(there)
        def _():
            pl.semaphore_signal(barrier, inc=1, device_id=(comp, other), device_id_type=MESH)

    if forward:
        high, rest = split(a_ref[...])
        wide[...] = jnp.concatenate([high, high], axis=1)
        low[...] = rest
    if backward:
        high, rest = split(a_ref[...].T)
        wide_t[...] = jnp.concatenate([high, high], axis=1)
        low_t[...] = rest
    total = forward + backward
    for side in (0, 1):

        @pl.when(jnp.logical_not(has[side]))
        def _():
            def clear(i, _):
                halo[i, side] = jnp.zeros((levels, lon), f32)
                return _

            lax.fori_loop(0, total, clear, 0)

    pl.semaphore_wait(barrier, has_up.astype(jnp.int32) + has_down.astype(jnp.int32))
    load.wait()
    for r in range(rows):
        first[r, 0:1, :] = first[r, 0:1, :] + add_ref[r : r + 1, :]

    def copy(h, slot, side, c):
        columns = pl.ds(c * width, width)
        return pltpu.make_async_remote_copy(
            src_ref=state.at[slot, (rows - 1) * side, :, columns],
            dst_ref=halo.at[h, 1 - side, :, columns],
            send_sem=send_sem.at[h, side, c],
            recv_sem=recv_sem.at[h, 1 - side, c],
            device_id=(comp, (up, down)[side]),
            device_id_type=MESH,
        )

    def send(h, slot, side, c):
        @pl.when(has[side])
        def _():
            copy(h, slot, side, c).start()

    def receive(h, slot, side, c):
        @pl.when(has[side])
        def _():
            copy(h, slot, 1 - side, c).wait_recv()

    def pieces():
        return [slice(k, k + SUB) for k in range(0, levels, SUB)]

    def stencil(now, above, below, k, cols):
        x = now[k, :]
        left, right = pltpu.roll(x, 1, axis=1), pltpu.roll(x, lon - 1, axis=1)
        around = (left + right)[:, cols] + (above[k, cols] + below[k, cols])
        return x[:, cols], around - 4.0 * x[:, cols]

    def forward_row(slot, r, above, below, cols, target):
        now = state.at[slot, r]
        sea = sea_ref[pl.ds(r, 1), :][:, cols]
        y = mix(wide[...], low[...], now[:, cols])
        for k in pieces():
            x, lap = stencil(now, above, below, k, cols)
            target[r, k, cols] = sea * (x + d_ref[r, k, cols] * lap + y[k])

    def scaled_row(slot, r, cols, k, adjoint):
        u = sea_ref[pl.ds(r, 1), :][:, cols] * adjoint
        masked[r, k, cols] = u
        state[slot, r, k, cols] = d_ref[r, k, cols] * u

    def backward_row(slot, r, above, below, cols, last):
        now = state.at[slot, r]
        y = mix(wide_t[...], low_t[...], masked[r, :, cols])
        for k in pieces():
            _, lap = stencil(now, above, below, k, cols)
            adjoint = masked[r, k, cols] + lap + y[k]
            if last:
                masked[r, k, cols] = adjoint if forward else adjoint + extra[r, k, cols]
            else:
                scaled_row(slot + 1, r, cols, k, adjoint)

    every = slice(0, lon)

    def step(h, slot, row, more):
        def inner(r, _):
            row(slot, r, state.at[slot, r - 1], state.at[slot, r + 1], every)
            return _

        lax.fori_loop(1, rows - 1, inner, 0)
        for c in range(CHUNKS):
            cols = slice(c * width, (c + 1) * width)
            for side in (0, 1):
                receive(h, slot, side, c)
                if side == 0:
                    row(slot, 0, halo.at[h, 0], state.at[slot, 1], cols)
                else:
                    row(slot, rows - 1, state.at[slot, rows - 2], halo.at[h, 1], cols)
                if more:
                    send(h + 1, slot + 1, side, c)

    def all_edges(h, slot):
        for c in range(CHUNKS):
            for side in (0, 1):
                send(h, slot, side, c)

    def run(base, slot0, count, make):
        def one(i, _):
            step(base + i, slot0 + i, make(False), True)
            return _

        lax.fori_loop(0, count - 1, one, 0)
        step(base + count - 1, slot0 + count - 1, make(True), False)

    base = 0
    slot0 = 0
    stores = []
    if forward:
        all_edges(0, 0)

        def make(last):
            return lambda slot, r, above, below, cols: forward_row(
                slot, r, above, below, cols, state.at[slot + 1]
            )

        run(0, 0, forward, make)
        base, slot0 = forward, forward + 1
        stores.append(pltpu.make_async_copy(state.at[forward], outs[0], io_sem.at[1]))
        stores[-1].start()
    if backward:

        def start_row(r, _):
            for k in pieces():
                if forward:
                    value = state[forward, r, k, :] - extra[r, k, :]
                else:
                    value = masked[r, k, :]
                scaled_row(slot0, r, every, k, value)
            return _

        start_row(0, 0)
        start_row(rows - 1, 0)
        all_edges(base, slot0)
        lax.fori_loop(1, rows - 1, start_row, 0)

        def make(last):
            return lambda slot, r, above, below, cols: backward_row(
                slot, r, above, below, cols, last
            )

        run(base, slot0, backward, make)
        stores.append(pltpu.make_async_copy(masked, outs[-1], io_sem.at[2]))
        stores[-1].start()
    for side in (0, 1):

        @pl.when(has[side])
        def _():
            for h in range(total):
                slot = h if h < forward else h + bool(forward)
                for c in range(CHUNKS):
                    copy(h, slot, side, c).wait_send()

    for store in stores:
        store.wait()


def run_block(tiles, ident, forward, backward, x, d, a, sea, add, extra=None):
    rows, levels, lon = x.shape
    total = forward + backward
    slots = (forward + 1 if forward else 0) + backward
    vmem = pl.BlockSpec(memory_space=pltpu.VMEM)
    hbm = pl.BlockSpec(memory_space=pl.ANY)
    operands = [x, d, a, sea, add] + ([extra] if extra is not None else [])
    outs = bool(forward) + bool(backward)
    scratch = [
        pltpu.VMEM((slots, rows, levels, lon), f32),
        pltpu.VMEM((total, 2, levels, lon), f32),
        pltpu.SemaphoreType.DMA((total, 2, CHUNKS)),
        pltpu.SemaphoreType.DMA((total, 2, CHUNKS)),
        pltpu.SemaphoreType.DMA((3,)),
        pltpu.VMEM((levels, 2 * levels), bf16),
        pltpu.VMEM((levels, levels), bf16),
    ]
    if backward:
        scratch += [
            pltpu.VMEM((rows, levels, lon), f32),
            pltpu.VMEM((levels, 2 * levels), bf16),
            pltpu.VMEM((levels, levels), bf16),
        ]
    return pl.pallas_call(
        functools.partial(block, tiles, forward, backward),
        out_shape=[jax.ShapeDtypeStruct(x.shape, f32)] * outs,
        in_specs=[hbm] + [vmem] * (len(operands) - 1),
        out_specs=[hbm] * outs,
        scratch_shapes=scratch,
        compiler_params=pltpu.CompilerParams(
            collective_id=ident, has_side_effects=True, vmem_limit_bytes=56 * 2**20
        ),
    )(*operands)


def swap_kernel(tiles, parcel, out, slots, send_sem, recv_sem):
    other, me = 1 - lax.axis_index("comp"), lax.axis_index("tile")
    barrier = pltpu.get_barrier_semaphore()
    for t in range(tiles):
        pl.semaphore_signal(barrier, inc=1, device_id=(other, t), device_id_type=MESH)
    pl.semaphore_wait(barrier, tiles)

    def copy(k, goes, lands):
        return pltpu.make_async_remote_copy(
            src_ref=parcel.at[goes],
            dst_ref=slots.at[lands],
            send_sem=send_sem.at[k],
            recv_sem=recv_sem.at[k],
            device_id=(other, goes),
            device_id_type=MESH,
        )

    for k in range(tiles):
        copy(k, lax.rem(me + k, tiles), me).start()
    for k in range(tiles):
        copy(k, lax.rem(me + k, tiles), lax.rem(me + tiles - k, tiles)).wait_recv()
    out[...] = slots[...]
    for k in range(tiles):
        copy(k, lax.rem(me + k, tiles), me).wait_send()


def swap(tiles, ident, parcel):
    vmem = pl.BlockSpec(memory_space=pltpu.VMEM)
    return pl.pallas_call(
        functools.partial(swap_kernel, tiles),
        out_shape=jax.ShapeDtypeStruct(parcel.shape, f32),
        in_specs=[vmem],
        out_specs=vmem,
        scratch_shapes=[
            pltpu.VMEM(parcel.shape, f32),
            pltpu.SemaphoreType.DMA((tiles,)),
            pltpu.SemaphoreType.DMA((tiles,)),
        ],
        compiler_params=pltpu.CompilerParams(collective_id=ident, has_side_effects=True),
    )(parcel)


def one_hot(index, count):
    return (index[:, None] == jnp.arange(count, dtype=jnp.int32)[None, :]).astype(f32)


def shards(
    starting_perturbation,
    measured_discrepancy,
    diffusion,
    vert_mix,
    ocean_mask,
    pair_tile,
    pair_patch,
    dest_patch,
    pair_blocks,
    remap_weight,
):
    component = lax.axis_index("comp")
    own_tile = lax.axis_index("tile")
    tiles = lax.axis_size("tile")
    row_count = starting_perturbation.shape[2]
    lon_count = starting_perturbation.shape[3]
    patch_len = remap_weight.shape[2]
    patch_count = row_count * lon_count // patch_len
    block_count = remap_weight.shape[1]
    pair_count = pair_tile.shape[2]
    per_pair = block_count // pair_count
    partner = 1 - component
    sea = jnp.where(component == 1, ocean_mask.astype(f32), 1.0)
    slot_ids = jnp.arange(block_count, dtype=jnp.int32) % per_pair
    own_tiles = jnp.repeat(pair_tile[component, own_tile], per_pair)
    live = (slot_ids < jnp.repeat(pair_blocks[0, 0], per_pair)).astype(f32)[:, None]
    landing = one_hot(dest_patch[0, 0], patch_count) * live
    weights = remap_weight[0]
    hits = (pair_tile[partner] == own_tile).astype(jnp.int32)
    feed = pair_patch[partner].reshape(tiles, pair_count, per_pair)
    send_rows = jnp.sum(hits[:, :, None] * feed, axis=1)
    sent = jnp.sum(hits, axis=1).astype(f32)
    sending = one_hot(send_rows.reshape(-1), patch_count) * jnp.repeat(sent, per_pair)[:, None]
    taking = one_hot(own_tiles * per_pair + slot_ids, tiles * per_pair)

    def to_rows(x):
        return jnp.swapaxes(x[0], 0, 1)

    start, measured, diff = map(
        to_rows, (starting_perturbation, measured_discrepancy, diffusion)
    )
    none = jnp.zeros((row_count, lon_count), f32)
    (middle,) = run_block(tiles, 0, STEPS, 0, start, diff, vert_mix[0], sea, none)

    surface = middle[:, 0].reshape(patch_count, patch_len)
    parcel = jnp.dot(sending, surface, precision=precise)
    arrived = swap(tiles, 1, parcel.reshape(tiles, per_pair, patch_len))
    picked = jnp.dot(taking, arrived.reshape(tiles * per_pair, patch_len), precision=precise)
    terms = jnp.sum(weights * picked[:, None, :], axis=2)
    summed = jnp.dot(landing.T, terms, precision=precise).reshape(row_count, lon_count)
    final, adjoint = run_block(
        tiles, 2, STEPS, STEPS, middle, diff, vert_mix[0], sea, sea * summed, measured
    )

    masked = sea.reshape(patch_count, patch_len) * adjoint[:, 0].reshape(patch_count, patch_len)
    spread = jnp.dot(landing, masked, precision=precise)
    terms = jnp.sum(weights * spread[:, :, None], axis=1)
    parcel = jnp.dot(taking.T, terms, precision=precise)
    back = swap(tiles, 3, parcel.reshape(tiles, per_pair, patch_len))
    returned = jnp.dot(sending.T, back.reshape(tiles * per_pair, patch_len), precision=precise)
    (last,) = run_block(
        tiles,
        4,
        0,
        STEPS,
        adjoint,
        diff,
        vert_mix[0],
        sea,
        returned.reshape(row_count, lon_count),
        start,
    )
    return (jnp.swapaxes(final, 0, 1)[None], jnp.swapaxes(last, 0, 1)[None])


def solution(mesh):
    placed = (
        P("comp", None, "tile", None),
        P("comp", None, "tile", None),
        P("comp", None, "tile", None),
        P("comp", None, None),
        P("tile", None),
        P(),
        P(),
        P("comp", "tile", None),
        P("comp", "tile", None),
        P("comp", "tile", None, None),
    )
    return jax.shard_map(
        shards,
        mesh=mesh,
        in_specs=placed,
        out_specs=(P("comp", None, "tile", None), P("comp", None, "tile", None)),
        check_vma=False,
    )
```
